32 devices in a mesh: group: 4 (over y, x), shard: 8 (over z, core).
Axes of the slice: x: 2, y: 2, z: 4, core: 2. Of those that a mesh axis runs over, the one named last changes fastest.
Arguments:
- inputs: bfloat16 [16384, 1024], P(('group', 'shard')), may hold values from -6 to 6
- cotangent: bfloat16 [16384, 1024], P(('group', 'shard')), may hold values from -6 to 6
- routes: int32 [16384, 2], P(('group', 'shard')), may hold values from 0 to 3, all different within a row
- priority: int32 [16384, 2], P(('group', 'shard')), may hold values from 0 to 1023, as said below
- buckets: int32 [1024], replicated, may hold values from 0 to 31
- norm1_gain: bfloat16 [1024], P(('group', 'shard')), may hold values from 0.5 to 1.5
- qkv_weight: bfloat16 [1024, 3072], P(('group', 'shard')), may hold values from -0.1875 to 0.1875
- out_weight: bfloat16 [1024, 1024], P(('group', 'shard')), may hold values from -0.75 to 0.75
- rel_bias: bfloat16 [512], P(('group', 'shard')), may hold values from -4 to 4
- norm2_gain: bfloat16 [1024], P(('group', 'shard')), may hold values from 0.5 to 1.5
- router_weight: bfloat16 [1024, 4], P(('group', 'shard')), may hold values from -0.375 to 0.375
- gate_weight: bfloat16 [4, 1024, 2816], P(None, ('group', 'shard')), may hold values from -0.1875 to 0.1875
- up_weight: bfloat16 [4, 1024, 2816], P(None, ('group', 'shard')), may hold values from -0.1875 to 0.1875
- down_weight: bfloat16 [4, 2816, 1024], P(None, ('group', 'shard')), may hold values from -0.3125 to 0.3125
Outputs:
- output: bfloat16 [16384, 1024], P(('group', 'shard'))
- input_grad: float32 [16384, 1024], P(('group', 'shard'))
- norm1_grad: float32 [1024], P('shard')
- qkv_grad: float32 [1024, 3072], P('shard')
- out_grad: float32 [1024, 1024], P('shard')
- rel_grad: float32 [512], P('shard')
- norm2_grad: float32 [1024], P('shard')
- router_grad: float32 [1024, 4], P('shard')
- gate_grad: float32 [4, 1024, 2816], P(None, 'shard')
- up_grad: float32 [4, 1024, 2816], P(None, 'shard')
- down_grad: float32 [4, 2816, 1024], P(None, None, 'shard')
The draws below stay inside these ranges and needn't reach their ends.
Inputs may be any that keep to these rules, and one draw needn't show every extreme that they name: `routes`: the two experts of a token differ. `priority`: within each aligned block of 512 rows (one device's tokens) the 1024 ranks are 0 to 1023, each once.
All inputs are finite; a program needn't handle non-finite values.
Results may differ from the reference program's by a relative error of at most 0.023.
Values may be sent and summed in bfloat16 or wider, within the bound.
A program may use at most 384 MiB of HBM per device.

```python
from functools import partial
import jax
import jax.numpy as jnp
from jax import lax

D = 1024
HEADS = 16
FF = 2816
BUCKETS = 32
EXPERTS = 4
SEQ_LEN = 1024
TOK_DEV = 512
CAP = 320
TOKENS = 16384


def draw_priority(key, part):
    block_count = TOKENS // TOK_DEV
    block_keys = jax.random.split(key, block_count)

    def shuffle_block(block_key):
        return jax.random.permutation(block_key, 2 * TOK_DEV)
    ranking = jax.vmap(shuffle_block)(block_keys)
    return ranking.reshape(TOKENS, 2).astype(jnp.int32)


def with_ends(array, stream_key, low, largest):
    longest = array.shape.index(max(array.shape))
    spots = []
    for shift in (0, 1):
        where = [jax.random.randint(jax.random.fold_in(stream_key, axis), (), 0, length) for axis, length in enumerate(array.shape)]
        where[longest] = (where[longest] + shift) % array.shape[longest]
        spots.append(tuple(where))
    return array.at[spots[0]].set(low).at[spots[1]].set(largest)


def steps_of(stream_key, shape, pieces, least, largest):
    def one(dim, parts):
        heights = jax.random.uniform(jax.random.fold_in(jax.random.fold_in(stream_key, 6), dim), (parts,), jnp.float32, least / len(pieces), largest / len(pieces))
        return jnp.repeat(jnp.exp(heights), shape[dim] // parts).reshape((-1,) + (1,) * (len(shape) - dim - 1))

    factor_of = one(*pieces[0])
    for cut in pieces[1:]:
        factor_of = factor_of * one(*cut)
    return factor_of


def choose_distinct(key, rows, amount, top, lift):
    order = jax.random.permutation(jax.random.fold_in(key, 1), amount)
    favour = order
    for power in range(3):
        favour = favour * favour // amount
    favour = favour * lift // amount
    chance = jax.random.randint(jax.random.fold_in(key, 2), (rows, amount), 0, 4096) + favour
    fixed_rows = jax.random.permutation(jax.random.fold_in(key, 3), rows)[jnp.arange(amount) % rows]
    chance = jnp.where(jnp.arange(rows)[:, None] == fixed_rows[None, :], 1 << 14, chance)
    merit = chance * amount + jnp.arange(amount)
    return lax.top_k(merit.astype(jnp.int32), top)[1].astype(jnp.int32)


def noise(own_key, extent, width, limit, pieces=(), kind=jnp.bfloat16):
    drawn = width * jax.random.normal(own_key, extent, jnp.float32)
    if pieces:
        drawn = drawn * steps_of(own_key, extent, pieces, -0.22, 0.18)
    return jnp.clip(drawn, -limit, limit).astype(kind)


def setup_inputs(seed: int = 0) -> dict:
    key_list = jax.random.split(jax.random.key(seed), 15)
    return {
        "inputs": noise(key_list[0], (TOKENS, D), 1.0, 6.0, ((0, 32),)),
        "cotangent": noise(key_list[1], (TOKENS, D), 1.0, 6.0, ((0, 32),)),
        "routes": choose_distinct(key_list[2], TOKENS, EXPERTS, 2, 4096),
        "priority": draw_priority(jax.random.fold_in(key_list[14], 71), 0),
        "buckets": with_ends(jax.random.randint(key_list[4], (SEQ_LEN,), 0, BUCKETS), jax.random.fold_in(key_list[4], 1), 0, BUCKETS - 1).astype(jnp.int32),
        "norm1_gain": jnp.clip(1.0 + 0.1 * jax.random.normal(key_list[5], (D,), jnp.float32), 0.5, 1.5).astype(jnp.bfloat16),
        "qkv_weight": noise(key_list[6], (D, 3 * D), D ** -0.5, 0.1875, ((0, 32),)),
        "out_weight": noise(key_list[7], (D, D), (D // 16) ** -0.5, 0.75, ((0, 32),)),
        "rel_bias": noise(key_list[8], (BUCKETS * HEADS,), 1.0, 4.0, ((0, 32),)),
        "norm2_gain": jnp.clip(1.0 + 0.1 * jax.random.normal(key_list[9], (D,), jnp.float32), 0.5, 1.5).astype(jnp.bfloat16),
        "router_weight": noise(key_list[10], (D, EXPERTS), (D // 4) ** -0.5, 0.375, ((0, 32),)),
        "gate_weight": noise(key_list[11], (EXPERTS, D, FF), D ** -0.5, 0.1875, ((1, 32),)),
        "up_weight": noise(key_list[12], (EXPERTS, D, FF), D ** -0.5, 0.1875, ((1, 32),)),
        "down_weight": noise(key_list[13], (EXPERTS, FF, D), (FF // 8) ** -0.5, 0.3125, ((1, 32),)),
    }


EPSILON = 1e-06
MASKED = -1e+30
PRECISE = lax.Precision.HIGHEST

@jax.custom_vjp
def low(v):
    return lax.optimization_barrier(v.astype(jnp.bfloat16)).astype(jnp.float32)

@jax.custom_vjp
def low_back(v):
    return v

def low_keep(v):
    return (low(v), None)

def low_pass(kept, grad):
    return (grad,)

def back_keep(v):
    return (v, None)

def back_low(kept, grad):
    return (low(grad),)
low.defvjp(low_keep, low_pass)
low_back.defvjp(back_keep, back_low)

def exact_dot(matrix_a, matrix_b):
    return jnp.dot(matrix_a, matrix_b, precision=PRECISE, preferred_element_type=jnp.float32)

def row_positions(length):
    quarter = length // 4
    rows = jnp.arange(length, dtype=jnp.int32)
    return jnp.where(rows < quarter, rows, jnp.where(rows < 2 * quarter, rows + 2 * quarter, rows - quarter)).astype(jnp.int32)

def scaled_norm(residual, norm_gain):
    inverse = lax.rsqrt(lax.optimization_barrier(jnp.mean(residual * residual, axis=-1, keepdims=True)) + EPSILON)
    return residual * inverse * norm_gain

def attention(normed, qkv_matrix, out_matrix, bias_table, buckets):
    length = normed.shape[0]
    model_width = normed.shape[1]
    head_count = bias_table.shape[1]
    head_dim = model_width // head_count
    projected = low_back(low(exact_dot(normed, qkv_matrix)))
    queries = projected[:, :model_width].reshape(length, head_count, head_dim)
    all_keys = projected[:, model_width:2 * model_width].reshape(length, head_count, head_dim)
    values = projected[:, 2 * model_width:].reshape(length, head_count, head_dim)
    position = row_positions(length)
    distance = position[:, None] - position[None, :]
    bucket_hot = (buckets[:, None] == jnp.arange(bias_table.shape[0], dtype=jnp.int32)[None, :]).astype(jnp.float32)
    per_dist = exact_dot(bucket_hot, bias_table)
    score_bias = jnp.transpose(per_dist)[:, jnp.clip(distance, 0, length - 1)]
    raw_scores = jnp.einsum('ihd,jhd->hij', queries, all_keys, precision=PRECISE) * head_dim ** (-0.5) + score_bias
    scores = jnp.where(distance[None] >= 0, low_back(raw_scores), MASKED)
    attn_probs = jax.nn.softmax(scores, axis=-1)
    attn_mixed = jnp.einsum('hij,jhd->ihd', low(attn_probs), values, precision=PRECISE).reshape(length, model_width)
    return low_back(exact_dot(low_back(low(attn_mixed)), out_matrix))

def moe_block(normed, block_routes, block_ranks, router_matrix, gate_stack, up_stack, down_stack):
    tokens = normed.shape[0]
    experts = gate_stack.shape[0]
    choices_all = 2 * tokens
    logits = low_back(exact_dot(normed, router_matrix))
    router_probs = jax.nn.softmax(logits, axis=-1)
    picked = jnp.take_along_axis(router_probs, block_routes, axis=1).reshape(choices_all)
    expert_of = block_routes.reshape(choices_all)
    expert_hot = (expert_of[:, None] == jnp.arange(experts, dtype=jnp.int32)[None, :]).astype(jnp.int32)
    ranking = block_ranks.reshape(choices_all)
    earlier = (ranking[None, :] < ranking[:, None]).astype(jnp.int32)
    slot_index = lax.optimization_barrier(jnp.sum(jnp.dot(earlier, expert_hot) * expert_hot, axis=1))
    kept_mask = slot_index < CAP
    slot_hot = ((slot_index[:, None] == jnp.arange(CAP, dtype=jnp.int32)[None, :]) & kept_mask[:, None]).astype(jnp.float32)
    dispatch = (expert_hot.astype(jnp.float32)[:, :, None] * slot_hot[:, None, :]).reshape(tokens, 2, experts, CAP)
    buffer = jnp.einsum('tec,td->ecd', lax.optimization_barrier(jnp.sum(dispatch, axis=1)), normed, precision=PRECISE)
    gate_act = low_back(jnp.einsum('ecd,edf->ecf', buffer, gate_stack, precision=PRECISE))
    up_act = low_back(jnp.einsum('ecd,edf->ecf', buffer, up_stack, precision=PRECISE))
    hidden = low(jax.nn.gelu(gate_act, approximate=True) * up_act)
    expert_out = low_back(jnp.einsum('ecf,efd->ecd', hidden, down_stack, precision=PRECISE))
    combine = lax.optimization_barrier(jnp.sum(dispatch * picked.reshape(tokens, 2)[:, :, None, None], axis=1))
    return jnp.einsum('tec,ecd->td', combine, expert_out, precision=PRECISE)

def layer(seq_in, seq_routes, seq_ranks, params, buckets):
    norm_first, qkv_matrix, out_matrix, bias_flat, norm_second, router_matrix, gate_stack, up_stack, down_stack = params
    normed_one = low(scaled_norm(seq_in, norm_first))
    resid_mid = seq_in + attention(normed_one, qkv_matrix, out_matrix, bias_flat.reshape(BUCKETS, HEADS), buckets)
    normed_two = low(scaled_norm(resid_mid, norm_second))
    blocks = SEQ_LEN // TOK_DEV
    mixture = jax.vmap(moe_block, in_axes=(0, 0, 0, None, None, None, None))(normed_two.reshape(blocks, TOK_DEV, D), seq_routes.reshape(blocks, TOK_DEV, 2), seq_ranks.reshape(blocks, TOK_DEV, 2), router_matrix, gate_stack, up_stack, down_stack)
    return resid_mid + mixture.reshape(SEQ_LEN, D)

def reference(inputs, cotangent, routes, priority, buckets, norm1_gain, qkv_weight, out_weight, rel_bias, norm2_gain, router_weight, gate_weight, up_weight, down_weight):
    weights = tuple((tensor.astype(jnp.float32) for tensor in (norm1_gain, qkv_weight, out_weight, rel_bias, norm2_gain, router_weight, gate_weight, up_weight, down_weight)))
    seq_count = TOKENS // SEQ_LEN
    seq_inputs = inputs.astype(jnp.float32).reshape(seq_count, SEQ_LEN, D)
    seq_routes = routes.reshape(seq_count, SEQ_LEN, 2)
    seq_ranks = priority.reshape(seq_count, SEQ_LEN, 2)
    checked = jax.checkpoint(partial(layer, buckets=buckets))

    def whole(seq_in, params):

        def one_sequence(loop_state, sequence):
            return (loop_state, checked(sequence[0], sequence[1], sequence[2], params))
        _, outputs = lax.scan(one_sequence, jnp.zeros((), jnp.float32), (seq_in, seq_routes, seq_ranks))
        return outputs
    result, pull = jax.vjp(whole, seq_inputs, weights)
    d_inputs, d_weights = pull(cotangent.astype(jnp.float32).reshape(seq_count, SEQ_LEN, D))
    return (result.reshape(TOKENS, D).astype(jnp.bfloat16), d_inputs.reshape(TOKENS, D), d_weights[0], d_weights[1], d_weights[2], d_weights[3], d_weights[4], d_weights[5], d_weights[6], d_weights[7], d_weights[8])
```

```python
import functools

import jax
import jax.numpy as jnp
from jax import lax
from jax.experimental import pallas as pl
from jax.experimental.pallas import tpu as pltpu
from jax.sharding import PartitionSpec as P

HEADS = 16
BUCKETS = 32
CAP = 320
EPSILON = 1e-06
MASKED = -1e30
F32 = jnp.float32
BF16 = jnp.bfloat16


def swap(value, axis, k):
    return lax.ppermute(value, axis, [(i, i ^ k) for i in range(lax.axis_size(axis))])


def bits_of(size):
    return [1 << b for b in range(size.bit_length() - 1)]


def nt(a, b, precision=None):
    return lax.dot_general(
        a, b, (((1,), (1,)), ((), ())), preferred_element_type=F32, precision=precision
    )


def nn(a, b):
    return lax.dot_general(a, b, (((1,), (0,)), ((), ())), preferred_element_type=F32)


def spread(u_ref, f_row):
    width = f_row.shape[1]
    u_ref[...] = pltpu.roll(
        jnp.broadcast_to(f_row, (128, width)), 0, 1, stride=1, stride_axis=0
    )


def toeplitz(u_ref, base):
    top = u_ref[:, pl.ds(pl.multiple_of(base + 256, 128), 256)]
    bottom = u_ref[:, pl.ds(pl.multiple_of(base + 128, 128), 256)]
    return jnp.concatenate([top, bottom], axis=0)


def head_lanes(h):
    lane = lax.broadcasted_iota(jnp.int32, (1, 128), 1)
    return (lane >= 64 * h) & (lane < 64 * h + 64)


def causal():
    row = lax.broadcasted_iota(jnp.int32, (256, 256), 0)
    col = lax.broadcasted_iota(jnp.int32, (256, 256), 1)
    return row <= col


def attention_forward_kernel(
    p_ref, q_ref, k_ref, v_ref, ko_ref, vo_ref, f_ref, o_ref, lse_ref, u_ref
):
    half = p_ref[0]
    first = half == 1
    off = pl.multiple_of((1 - half) * 256, 256)
    base3 = pl.multiple_of(768 - half * 512, 256)
    q = q_ref[...].astype(F32) * 0.125
    keep = causal()
    vt = v_ref[...].T
    vot = vo_ref[pl.ds(0, 256), :].T
    v5t = vo_ref[pl.ds(off, 256), :].T
    ka, kb = k_ref[pl.ds(0, 256), :], k_ref[pl.ds(256, 256), :]
    ko0, k5 = ko_ref[pl.ds(0, 256), :], ko_ref[pl.ds(off, 256), :]
    out_a, out_b = [], []
    for h in range(2):
        spread(u_ref, f_ref[0, h : h + 1, :])
        qh = jnp.where(head_lanes(h), q, 0.0).astype(BF16)
        qa, qb = qh[:256], qh[256:]
        q5 = jnp.where(first, qa, qb)
        t0 = toeplitz(u_ref, 0)
        s1 = jnp.where(keep, nt(ka, qa) + t0, MASKED)
        s2 = jnp.where(keep, nt(kb, qb) + t0, MASKED)
        s3 = nt(ka, qb) + toeplitz(u_ref, base3)
        s4 = nt(ko0, qb) + toeplitz(u_ref, 512)
        s5 = nt(k5, q5) + toeplitz(u_ref, 256)
        m1, m2, m3, m4, m5 = [jnp.max(s, axis=0, keepdims=True) for s in (s1, s2, s3, s4, s5)]
        ma = jnp.maximum(m1, jnp.where(first, m5, MASKED))
        mb = jnp.maximum(jnp.maximum(m2, m3), m4)
        mb = jnp.maximum(mb, jnp.where(first, MASKED, m5))
        p1 = jnp.exp(s1 - ma)
        p2 = jnp.exp(s2 - mb)
        p3 = jnp.exp(s3 - mb)
        p4 = jnp.exp(s4 - mb)
        p5 = jnp.exp(s5 - jnp.where(first, ma, mb))
        l1, l2, l3, l4, l5 = [jnp.sum(p, axis=0, keepdims=True) for p in (p1, p2, p3, p4, p5)]
        la = l1 + jnp.where(first, l5, 0.0)
        lb = l2 + l3 + l4 + jnp.where(first, 0.0, l5)
        rows = slice(64 * h, 64 * h + 64)
        o5 = nn(v5t[rows], p5.astype(BF16))
        oa = nn(vt[rows, :256], p1.astype(BF16)) + jnp.where(first, o5, 0.0)
        ob = (
            nn(vt[rows, 256:], p2.astype(BF16))
            + nn(vt[rows, :256], p3.astype(BF16))
            + nn(vot[rows], p4.astype(BF16))
            + jnp.where(first, 0.0, o5)
        )
        out_a.append(oa / la)
        out_b.append(ob / lb)
        lse_ref[0, h : h + 1, pl.ds(0, 256)] = ma + jnp.log(la)
        lse_ref[0, h : h + 1, pl.ds(256, 256)] = mb + jnp.log(lb)
    o_ref[pl.ds(0, 256), :] = jnp.concatenate(out_a, axis=0).T.astype(BF16)
    o_ref[pl.ds(256, 256), :] = jnp.concatenate(out_b, axis=0).T.astype(BF16)


def attention_backward_kernel(
    p_ref,
    q_ref,
    k_ref,
    v_ref,
    ko_ref,
    vo_ref,
    do_ref,
    o_ref,
    lse_ref,
    f_ref,
    dq_ref,
    dk_ref,
    dv_ref,
    dko_ref,
    dvo_ref,
    g_ref,
    u_ref,
    acc_ref,
    dk_s,
    dv_s,
):
    half = p_ref[0]
    first = half == 1
    off = pl.multiple_of((1 - half) * 256, 256)
    base3 = pl.multiple_of(768 - half * 512, 256)
    q = q_ref[...].astype(F32) * 0.125
    do = do_ref[...].astype(F32)
    keep = causal()
    kt = k_ref[...].T
    kot = ko_ref[pl.ds(0, 256), :].T
    k5t = ko_ref[pl.ds(off, 256), :].T
    dk_s[...] = jnp.zeros_like(dk_s)
    dv_s[...] = jnp.zeros_like(dv_s)
    row8 = lax.broadcasted_iota(jnp.int32, (8, 128), 0)
    lane8 = lax.broadcasted_iota(jnp.int32, (8, 128), 1)
    ones = jnp.where(lane8 // 64 == row8, 1.0, 0.0)
    deltas = nt(ones, do * o_ref[...].astype(F32), precision=lax.Precision.HIGHEST)
    dqt_a, dqt_b = [], []
    for h in range(2):
        spread(u_ref, f_ref[0, h : h + 1, :])
        acc_ref[...] = jnp.zeros_like(acc_ref)
        qh = jnp.where(head_lanes(h), q, 0.0).astype(BF16)
        dh = jnp.where(head_lanes(h), do, 0.0).astype(BF16)
        lse = lse_ref[0, h : h + 1, :]
        delta = deltas[h : h + 1, :]
        rows = slice(64 * h, 64 * h + 64)

        def block(k, v, key_rows, k_t, qs, ds, l, d, base, masked):
            s = nt(k, qs) + toeplitz(u_ref, base)
            p = jnp.exp(s - l)
            if masked:
                p = jnp.where(keep, p, 0.0)
            e = p * (nt(v, ds) - d)
            acc_ref[:, pl.ds(pl.multiple_of(base + 256, 128), 256)] += e[:128]
            acc_ref[:, pl.ds(pl.multiple_of(base + 128, 128), 256)] += e[128:]
            el = e.astype(BF16)
            dv_s[key_rows, :] += nn(p.astype(BF16), ds)
            dk_s[key_rows, :] += nn(el, qs)
            return nn(k_t[rows], el)

        ka, kb = k_ref[pl.ds(0, 256), :], k_ref[pl.ds(256, 256), :]
        va, vb = v_ref[pl.ds(0, 256), :], v_ref[pl.ds(256, 256), :]
        qa, qb, da, db = qh[:256], qh[256:], dh[:256], dh[256:]
        la, lb, ea, eb = lse[:, :256], lse[:, 256:], delta[:, :256], delta[:, 256:]
        t1 = block(ka, va, pl.ds(0, 256), kt[:, :256], qa, da, la, ea, 0, True)
        t2 = block(kb, vb, pl.ds(256, 256), kt[:, 256:], qb, db, lb, eb, 0, True)
        t3 = block(ka, va, pl.ds(0, 256), kt[:, :256], qb, db, lb, eb, base3, False)
        t4 = block(
            ko_ref[pl.ds(0, 256), :],
            vo_ref[pl.ds(0, 256), :],
            pl.ds(512, 256),
            kot,
            qb,
            db,
            lb,
            eb,
            512,
            False,
        )
        t5 = block(
            ko_ref[pl.ds(off, 256), :],
            vo_ref[pl.ds(off, 256), :],
            pl.ds(pl.multiple_of(512 + off, 256), 256),
            k5t,
            jnp.where(first, qa, qb),
            jnp.where(first, da, db),
            jnp.where(first, la, lb),
            jnp.where(first, ea, eb),
            256,
            False,
        )
        dqt_a.append(t1 + jnp.where(first, t5, 0.0))
        dqt_b.append(t2 + t3 + t4 + jnp.where(first, 0.0, t5))
        x = acc_ref[...]
        width = x.shape[1]
        for r in (64, 32, 16, 8):
            x = x[:r] + pltpu.roll(x[r : 2 * r], width - r, 1)
        for r in (4, 2, 1):
            x = x + pltpu.roll(pltpu.roll(x, 8 - r, 0), width - r, 1)
        g_ref[0, h : h + 1, :] = x[0:1]
    dq_ref[pl.ds(0, 256), :] = (jnp.concatenate(dqt_a, axis=0).T * 0.125).astype(BF16)
    dq_ref[pl.ds(256, 256), :] = (jnp.concatenate(dqt_b, axis=0).T * 0.125).astype(BF16)
    dk_ref[...] = dk_s[pl.ds(0, 512), :]
    dv_ref[...] = dv_s[pl.ds(0, 512), :]
    dko_ref[...] = dk_s[pl.ds(512, 512), :].astype(BF16)
    dvo_ref[...] = dv_s[pl.ds(512, 512), :].astype(BF16)


def attention_specs(tokens, pairs):
    def at(column):
        return pl.BlockSpec((tokens, 128), lambda i, p, c=column: (0, c + i))

    def table(width):
        return pl.BlockSpec((1, 8, width), lambda i, p: (i, 0, 0))

    return at, table


def attention_forward(half, projected, other, distances):
    tokens, width = projected.shape[0], projected.shape[1] // 3
    pairs = width // 128
    at, table = attention_specs(tokens, pairs)
    return pl.pallas_call(
        attention_forward_kernel,
        grid_spec=pltpu.PrefetchScalarGridSpec(
            num_scalar_prefetch=1,
            grid=(pairs,),
            in_specs=[at(0), at(pairs), at(2 * pairs), at(0), at(pairs), table(1280)],
            out_specs=[at(0), table(tokens)],
            scratch_shapes=[pltpu.VMEM((128, 1280), F32)],
        ),
        out_shape=[
            jax.ShapeDtypeStruct((tokens, width), BF16),
            jax.ShapeDtypeStruct((pairs, 8, tokens), F32),
        ],
        cost_estimate=pl.CostEstimate(
            flops=int(4e9), bytes_accessed=6 << 20, transcendentals=tokens * 1024 * 10
        ),
        name="attention_forward",
    )(half, projected, projected, projected, other, other, distances)


def attention_backward(half, projected, other, d_mixed, mixed, lse, distances):
    tokens, width = mixed.shape
    pairs = width // 128
    at, table = attention_specs(tokens, pairs)
    wide = jax.ShapeDtypeStruct((tokens, width), F32)
    low = jax.ShapeDtypeStruct((tokens, width), BF16)
    return pl.pallas_call(
        attention_backward_kernel,
        grid_spec=pltpu.PrefetchScalarGridSpec(
            num_scalar_prefetch=1,
            grid=(pairs,),
            in_specs=[
                at(0),
                at(pairs),
                at(2 * pairs),
                at(0),
                at(pairs),
                at(0),
                at(0),
                table(tokens),
                table(1280),
            ],
            out_specs=[at(0)] * 5 + [table(1280)],
            scratch_shapes=[
                pltpu.VMEM((128, 1280), F32),
                pltpu.VMEM((128, 1280), F32),
                pltpu.VMEM((2 * tokens, 128), F32),
                pltpu.VMEM((2 * tokens, 128), F32),
            ],
        ),
        out_shape=[low, wide, wide, low, low, jax.ShapeDtypeStruct((pairs, 8, 1280), F32)],
        cost_estimate=pl.CostEstimate(
            flops=int(12e9), bytes_accessed=12 << 20, transcendentals=tokens * 1024 * 10
        ),
        name="attention_backward",
    )(half, projected, projected, projected, other, other, d_mixed, mixed, lse, distances)


def gather_column(piece, axis):
    size = lax.axis_size(axis)
    me = lax.axis_index(axis)
    pieces = {0: piece}
    for bit in reversed(bits_of(size)):
        pieces.update({k | bit: swap(v, axis, bit) for k, v in list(pieces.items())})
    sources, rows, columns = piece.shape
    whole = jnp.zeros((sources, size, rows, columns), piece.dtype)
    for k, v in pieces.items():
        whole = lax.dynamic_update_slice(whole, v[:, None], (0, me ^ k, 0, 0))
    return whole.reshape(sources * size * rows, columns)


def to_experts(weight, experts):
    groups = lax.axis_size("group")
    sets = [[s * experts + i for i in range(experts)] for s in range(groups // experts)]
    moved = lax.all_to_all(
        weight,
        "group",
        split_axis=0,
        concat_axis=0,
        tiled=True,
        axis_index_groups=sets if len(sets) > 1 else None,
    )
    bit = experts
    me = lax.axis_index("group")
    while bit < groups:
        other = swap(moved, "group", bit)
        low = (me & bit) == 0
        moved = jnp.where(
            low, jnp.concatenate([moved, other]), jnp.concatenate([other, moved])
        )
        bit *= 2
    return moved


def pair_split(x, axis, width, bit_set):
    count = x.shape[axis] // width
    if axis == 0:
        view = x.reshape(count // 2, 2, width, *x.shape[1:])

        def half(bit):
            return lax.dynamic_index_in_dim(view, bit, 1, keepdims=False).reshape(
                count // 2 * width, *x.shape[1:]
            )

        return half(bit_set), half(1 - bit_set)

    def columns(bit):
        return jnp.concatenate(
            [
                lax.dynamic_slice_in_dim(x, (2 * m + bit) * width, width, axis)
                for m in range(count // 2)
            ],
            axis=axis,
        )

    return columns(bit_set), columns(1 - bit_set)


def halve(x, mesh_axis, bit, axis, width):
    me = lax.axis_index(mesh_axis)
    mine, theirs = pair_split(x, axis, width, jnp.where((me & bit) == 0, 0, 1))
    return (mine.astype(F32) + swap(theirs, mesh_axis, bit).astype(F32)).astype(x.dtype)


def reduce_column(grad, axis, width):
    for bit in bits_of(lax.axis_size("shard")):
        grad = halve(grad, "shard", bit, axis, width)
    return grad


def share_experts(part, experts):
    groups = lax.axis_size("group")
    me = lax.axis_index("group")
    bit = experts
    while bit < groups:
        part = (part.astype(F32) + swap(part, "group", bit).astype(F32)).astype(part.dtype)
        bit *= 2
    whole = jnp.zeros((experts, *part.shape), F32)
    mine = me % experts
    for k in range(experts):
        got = part if k == 0 else swap(part, "group", k)
        whole = lax.dynamic_update_slice(
            whole, got.astype(F32)[None], (mine ^ k,) + (0,) * part.ndim
        )
    return whole


def reduce_dense(grad):
    shards = lax.axis_size("shard")
    groups = lax.axis_size("group")
    me = lax.axis_index("group")
    rows, columns = grad.shape
    width = rows // shards
    sub = width // groups
    x = halve(grad, "shard", 1, 0, width)
    view = x.reshape(shards // 2, groups, sub, columns)

    def part(which):
        return lax.dynamic_index_in_dim(view, which, 1, keepdims=False)

    total = part(me).astype(F32)
    for k in range(1, groups):
        total = total + swap(part(me ^ k), "group", k).astype(F32)
    x = total.astype(BF16).reshape(shards // 2 * sub, columns)
    for bit in bits_of(shards)[1:]:
        x = halve(x, "shard", bit, 0, sub)
    whole = jnp.zeros((groups, sub, columns), F32)
    for k in range(groups):
        got = x if k == 0 else swap(x, "group", k)
        whole = lax.dynamic_update_slice(whole, got.astype(F32)[None], (me ^ k, 0, 0))
    return whole.reshape(width, columns)


def exchange(blocks, experts):
    return [blocks[0]] + [swap(blocks[k], "group", k) for k in range(1, experts)]


def norm_parts(x):
    inverse = lax.rsqrt(jnp.mean(x * x, axis=-1, keepdims=True) + EPSILON)
    return inverse


def norm_backward(d_out, x, inverse, gain):
    unit = x * inverse
    scaled = d_out * gain
    d_x = inverse * (scaled - unit * jnp.mean(scaled * unit, axis=-1, keepdims=True))
    return d_x, jnp.sum(d_out * unit, axis=0)


def gelu_parts(v):
    c = 0.7978845608028654
    t = jnp.tanh(c * (v + 0.044715 * v * v * v))
    value = 0.5 * v * (1.0 + t)
    slope = 0.5 * (1.0 + t) + 0.5 * v * (1.0 - t * t) * c * (1.0 + 3 * 0.044715 * v * v)
    return value, slope


def on_device(
    inputs,
    cotangent,
    routes,
    priority,
    buckets,
    norm1_gain,
    qkv_weight,
    out_weight,
    rel_bias,
    norm2_gain,
    router_weight,
    gate_weight,
    up_weight,
    down_weight,
):
    tokens, width = inputs.shape
    experts = gate_weight.shape[0]
    ff = gate_weight.shape[2]
    both = ("group", "shard")
    devices = lax.axis_size("group") * lax.axis_size("shard")
    rows = qkv_weight.shape[0]
    shards = lax.axis_size("shard")

    bias_rows = jnp.zeros((rows, 1), BF16)
    bias_rows = jnp.pad(rel_bias.reshape(-1, 1), ((0, rows - rel_bias.shape[0]), (0, 0)))
    small = jnp.concatenate(
        [
            norm1_gain.reshape(rows, 1),
            norm2_gain.reshape(rows, 1),
            router_weight,
            bias_rows,
            jnp.zeros((rows, 128 - 3 - experts), BF16),
        ],
        axis=1,
    )
    small_full = lax.all_gather(small, both, axis=0, tiled=True)
    qkv_full = lax.all_gather(qkv_weight, both, axis=0, tiled=True)
    out_full = lax.all_gather(out_weight, both, axis=0, tiled=True)
    gate_up = to_experts(jnp.concatenate([gate_weight, up_weight], axis=1), experts)
    down_own = to_experts(down_weight, experts)
    gate_full = gather_column(gate_up[:, :rows], "shard")
    up_full = gather_column(gate_up[:, rows:], "shard")
    down_full = gather_column(down_own, "shard")

    small_f32 = small_full.astype(F32)
    gain_one = small_f32[:, 0].reshape(1, width)
    gain_two = small_f32[:, 1].reshape(1, width)
    router_full = small_full[:, 2 : 2 + experts]
    per_device = rel_bias.shape[0]
    table = small_full[:, 2 + experts].reshape(devices, rows)[:, :per_device]
    table = table.reshape(BUCKETS, HEADS)

    padded = jnp.concatenate([jnp.full((256,), -1, jnp.int32), buckets])
    bucket_hot = padded[:, None] == jnp.arange(BUCKETS, dtype=jnp.int32)[None, :]
    distances = jnp.einsum(
        "bh,nb->hn", table, bucket_hot.astype(BF16), preferred_element_type=F32
    ).reshape(HEADS // 2, 2, 1280)
    distances = jnp.pad(distances, ((0, 0), (0, 6), (0, 0)))

    group = lax.axis_index("group")
    choices = 2 * tokens
    expert_of = routes.reshape(choices)
    ranking = priority.reshape(choices)
    expert_hot = expert_of[:, None] == jnp.arange(experts, dtype=jnp.int32)[None, :]
    earlier = (ranking[None, :] < ranking[:, None]).astype(BF16)
    counts = jnp.dot(earlier, expert_hot.astype(BF16), preferred_element_type=F32)
    slot = jnp.sum(jnp.where(expert_hot, counts, 0.0), axis=1).astype(jnp.int32)
    kept = slot < CAP
    slots = experts * CAP
    place = jnp.where(kept, (expert_of ^ (group % experts)) * CAP + slot, -1)
    place = place.reshape(tokens, 2)
    kept = kept.reshape(tokens, 2)
    slot_ids = jnp.arange(slots, dtype=jnp.int32)
    hot_rows = [place[:, c][:, None] == slot_ids[None, :] for c in range(2)]

    resid_in = inputs.astype(F32)
    inverse_one = norm_parts(resid_in)
    normed_one = (resid_in * inverse_one * gain_one).astype(BF16)
    projected = jnp.dot(normed_one, qkv_full, preferred_element_type=F32).astype(BF16)
    half = (lax.axis_index("shard") % 2).astype(jnp.int32).reshape(1)
    other = swap(projected[:, width:], "shard", 1)
    mixed, lse = attention_forward(half, projected, other, distances)
    resid_mid = resid_in + jnp.dot(mixed, out_full, preferred_element_type=F32)
    inverse_two = norm_parts(resid_mid)
    normed_two = (resid_mid * inverse_two * gain_two).astype(BF16)

    logits = jnp.dot(normed_two, router_full, preferred_element_type=F32)
    router_probs = jax.nn.softmax(logits, axis=1)
    route_hot = routes[:, :, None] == jnp.arange(experts, dtype=jnp.int32)[None, None, :]
    picked = jnp.sum(jnp.where(route_hot, router_probs[:, None, :], 0.0), axis=2)
    gates = jnp.where(kept, picked, 0.0)

    dispatch = (hot_rows[0] | hot_rows[1]).astype(BF16)
    buffer = jnp.einsum(
        "ts,td->sd", dispatch, normed_two, preferred_element_type=F32
    ).astype(BF16)
    slot_gates = jnp.sum(
        jnp.where(hot_rows[0], gates[:, 0:1], 0.0) + jnp.where(hot_rows[1], gates[:, 1:2], 0.0),
        axis=0,
    )
    d_slots = (
        jnp.einsum("ts,td->sd", dispatch, cotangent, preferred_element_type=F32)
        * slot_gates[:, None]
    ).astype(BF16)
    blocks = buffer.reshape(experts, CAP, width)
    x = jnp.concatenate(exchange(blocks, experts), axis=0)
    d_expert = jnp.concatenate(exchange(d_slots.reshape(experts, CAP, width), experts), axis=0)

    gate_act = jnp.dot(x, gate_full, preferred_element_type=F32)
    up_act = jnp.dot(x, up_full, preferred_element_type=F32)
    gate_low, up_low = gate_act.astype(BF16), up_act.astype(BF16)
    hidden = (gelu_parts(gate_act)[0] * up_act).astype(BF16)
    expert_out = jnp.dot(hidden, down_full, preferred_element_type=F32).astype(BF16)
    returned = jnp.concatenate(
        exchange(expert_out.reshape(experts, CAP, width), experts), axis=0
    )
    down_grad = jnp.einsum(
        "sf,sd->fd", hidden, d_expert, preferred_element_type=F32
    ).astype(BF16)
    d_hidden = jnp.einsum("sd,fd->sf", d_expert, down_full, preferred_element_type=F32)
    value, slope = gelu_parts(gate_low.astype(F32))
    d_gate = (d_hidden * up_low.astype(F32) * slope).astype(BF16)
    d_up = (d_hidden * value).astype(BF16)
    d_buffer = (
        jnp.einsum("sf,df->sd", d_gate, gate_full, preferred_element_type=F32)
        + jnp.einsum("sf,df->sd", d_up, up_full, preferred_element_type=F32)
    ).astype(BF16)
    d_returned = jnp.concatenate(
        exchange(d_buffer.reshape(experts, CAP, width), experts), axis=0
    )
    gate_grad = jnp.einsum("sd,sf->df", x, d_gate, preferred_element_type=F32).astype(BF16)
    up_grad = jnp.einsum("sd,sf->df", x, d_up, preferred_element_type=F32).astype(BF16)
    part = width // shards
    down_out = share_experts(reduce_column(down_grad, 1, part), experts)
    gate_out = share_experts(reduce_column(gate_grad, 0, part), experts)
    up_out = share_experts(reduce_column(up_grad, 0, part), experts)

    grad_out = cotangent.astype(F32)
    mixture = jnp.zeros((tokens, width), F32)
    d_gates = []
    for c in range(2):
        rows_out = jnp.dot(hot_rows[c].astype(BF16), returned, preferred_element_type=F32)
        mixture = mixture + rows_out * gates[:, c : c + 1]
        d_gates.append(jnp.sum(grad_out * rows_out, axis=1))
    output = (resid_mid + mixture).astype(BF16)
    d_gates = jnp.stack(d_gates, axis=1)
    d_router = jnp.sum(jnp.where(route_hot, d_gates[:, :, None], 0.0), axis=1)
    d_logits = (
        router_probs * (d_router - jnp.sum(router_probs * d_router, axis=1, keepdims=True))
    ).astype(BF16)
    router_grad = jnp.einsum("td,te->ed", normed_two, d_logits, preferred_element_type=F32)
    d_normed_two = jnp.dot(dispatch, d_returned, preferred_element_type=F32) + jnp.einsum(
        "te,de->td", d_logits, router_full, preferred_element_type=F32
    )
    d_mid, gain_two_grad = norm_backward(d_normed_two, resid_mid, inverse_two, gain_two)
    d_resid_mid = grad_out + d_mid
    d_attn = d_resid_mid.astype(BF16)
    out_grad = reduce_dense(
        jnp.einsum("td,te->de", mixed, d_attn, preferred_element_type=F32).astype(BF16)
    )
    d_mixed = jnp.einsum("te,de->td", d_attn, out_full, preferred_element_type=F32).astype(BF16)
    dq, dk, dv, dk_other, dv_other, by_distance = attention_backward(
        half, projected, other, d_mixed, mixed, lse, distances
    )
    dk_back, dv_back = swap(dk_other, "shard", 1), swap(dv_other, "shard", 1)
    d_projected = jnp.concatenate(
        [dq, (dk + dk_back.astype(F32)).astype(BF16), (dv + dv_back.astype(F32)).astype(BF16)],
        axis=1,
    )
    qkv_grad = reduce_dense(
        jnp.einsum("td,te->de", normed_one, d_projected, preferred_element_type=F32).astype(BF16)
    )
    d_normed_one = jnp.einsum("te,de->td", d_projected, qkv_full, preferred_element_type=F32)
    d_in, gain_one_grad = norm_backward(d_normed_one, resid_in, inverse_one, gain_one)
    input_grad = d_resid_mid + d_in

    table_grad = jnp.einsum(
        "hn,nb->bh",
        by_distance[:, :2].reshape(HEADS, 1280),
        bucket_hot.astype(F32),
        preferred_element_type=F32,
        precision=lax.Precision.HIGHEST,
    ).reshape(1, BUCKETS * HEADS)
    packed = jnp.concatenate(
        [
            gain_one_grad.reshape(1, width),
            gain_two_grad.reshape(1, width),
            router_grad,
            jnp.pad(table_grad, ((0, 0), (0, width - BUCKETS * HEADS))),
            jnp.zeros((8 - 3 - experts, width), F32),
        ],
        axis=0,
    )
    packed = lax.psum(packed, both)
    shard = lax.axis_index("shard")
    own = lax.dynamic_slice_in_dim(packed, shard * part, part, 1)
    per_shard = BUCKETS * HEADS // shards
    rel_grad = lax.dynamic_slice(packed, (2 + experts, shard * per_shard), (1, per_shard))
    return (
        output,
        input_grad,
        own[0],
        qkv_grad,
        out_grad,
        rel_grad.reshape(per_shard),
        own[1],
        own[2 : 2 + experts].T,
        gate_out,
        up_out,
        down_out,
    )


def solution(mesh):
    return jax.shard_map(
        on_device,
        mesh=mesh,
        in_specs=(
            P(("group", "shard"), None),
            P(("group", "shard"), None),
            P(("group", "shard"), None),
            P(("group", "shard"), None),
            P(),
            P(("group", "shard")),
            P(("group", "shard"), None),
            P(("group", "shard"), None),
            P(("group", "shard")),
            P(("group", "shard")),
            P(("group", "shard"), None),
            P(None, ("group", "shard"), None),
            P(None, ("group", "shard"), None),
            P(None, ("group", "shard"), None),
        ),
        out_specs=(
            P(("group", "shard"), None),
            P(("group", "shard"), None),
            P("shard"),
            P("shard", None),
            P("shard", None),
            P("shard"),
            P("shard"),
            P("shard", None),
            P(None, "shard", None),
            P(None, "shard", None),
            P(None, None, "shard"),
        ),
        check_vma=False,
    )
```

```python
import functools

import jax
import jax.numpy as jnp
from jax import lax
from jax.experimental import pallas as pl
from jax.experimental.pallas import tpu as pltpu
from jax.sharding import PartitionSpec as P

HEADS = 16
BUCKETS = 32
CAP = 320
EPSILON = 1e-06
MASKED = -1e30
F32 = jnp.float32
BF16 = jnp.bfloat16


def swap(value, axis, k):
    return lax.ppermute(value, axis, [(i, i ^ k) for i in range(lax.axis_size(axis))])


def bits_of(size):
    return [1 << b for b in range(size.bit_length() - 1)]


def nt(a, b, precision=None):
    return lax.dot_general(
        a, b, (((1,), (1,)), ((), ())), preferred_element_type=F32, precision=precision
    )


def nn(a, b):
    return lax.dot_general(a, b, (((1,), (0,)), ((), ())), preferred_element_type=F32)


def spread(u_ref, f_row):
    width = f_row.shape[1]
    u_ref[...] = pltpu.roll(
        jnp.broadcast_to(f_row, (128, width)), 0, 1, stride=1, stride_axis=0
    )


def toeplitz(u_ref, base):
    top = u_ref[:, pl.ds(pl.multiple_of(base + 256, 128), 256)]
    bottom = u_ref[:, pl.ds(pl.multiple_of(base + 128, 128), 256)]
    return jnp.concatenate([top, bottom], axis=0)


def head_lanes(h):
    lane = lax.broadcasted_iota(jnp.int32, (1, 128), 1)
    return (lane >= 64 * h) & (lane < 64 * h + 64)


def causal():
    row = lax.broadcasted_iota(jnp.int32, (256, 256), 0)
    col = lax.broadcasted_iota(jnp.int32, (256, 256), 1)
    return row <= col


def attention_forward_kernel(
    p_ref, q_ref, k_ref, v_ref, ko_ref, vo_ref, f_ref, o_ref, lse_ref, u_ref
):
    half = p_ref[0]
    first = half == 1
    off = pl.multiple_of((1 - half) * 256, 256)
    base3 = pl.multiple_of(768 - half * 512, 256)
    q = q_ref[...].astype(F32) * 0.125
    keep = causal()
    vt = v_ref[...].T
    vot = vo_ref[pl.ds(0, 256), :].T
    v5t = vo_ref[pl.ds(off, 256), :].T
    ka, kb = k_ref[pl.ds(0, 256), :], k_ref[pl.ds(256, 256), :]
    ko0, k5 = ko_ref[pl.ds(0, 256), :], ko_ref[pl.ds(off, 256), :]
    out_a, out_b = [], []
    for h in range(2):
        spread(u_ref, f_ref[0, h : h + 1, :])
        qh = jnp.where(head_lanes(h), q, 0.0).astype(BF16)
        qa, qb = qh[:256], qh[256:]
        q5 = jnp.where(first, qa, qb)
        t0 = toeplitz(u_ref, 0)
        s1 = jnp.where(keep, nt(ka, qa) + t0, MASKED)
        s2 = jnp.where(keep, nt(kb, qb) + t0, MASKED)
        s3 = nt(ka, qb) + toeplitz(u_ref, base3)
        s4 = nt(ko0, qb) + toeplitz(u_ref, 512)
        s5 = nt(k5, q5) + toeplitz(u_ref, 256)
        m1, m2, m3, m4, m5 = [jnp.max(s, axis=0, keepdims=True) for s in (s1, s2, s3, s4, s5)]
        ma = jnp.maximum(m1, jnp.where(first, m5, MASKED))
        mb = jnp.maximum(jnp.maximum(m2, m3), m4)
        mb = jnp.maximum(mb, jnp.where(first, MASKED, m5))
        p1 = jnp.exp(s1 - ma)
        p2 = jnp.exp(s2 - mb)
        p3 = jnp.exp(s3 - mb)
        p4 = jnp.exp(s4 - mb)
        p5 = jnp.exp(s5 - jnp.where(first, ma, mb))
        l1, l2, l3, l4, l5 = [jnp.sum(p, axis=0, keepdims=True) for p in (p1, p2, p3, p4, p5)]
        la = l1 + jnp.where(first, l5, 0.0)
        lb = l2 + l3 + l4 + jnp.where(first, 0.0, l5)
        rows = slice(64 * h, 64 * h + 64)
        o5 = nn(v5t[rows], p5.astype(BF16))
        oa = nn(vt[rows, :256], p1.astype(BF16)) + jnp.where(first, o5, 0.0)
        ob = (
            nn(vt[rows, 256:], p2.astype(BF16))
            + nn(vt[rows, :256], p3.astype(BF16))
            + nn(vot[rows], p4.astype(BF16))
            + jnp.where(first, 0.0, o5)
        )
        out_a.append(oa / la)
        out_b.append(ob / lb)
        lse_ref[0, h : h + 1, pl.ds(0, 256)] = ma + jnp.log(la)
        lse_ref[0, h : h + 1, pl.ds(256, 256)] = mb + jnp.log(lb)
    o_ref[pl.ds(0, 256), :] = jnp.concatenate(out_a, axis=0).T.astype(BF16)
    o_ref[pl.ds(256, 256), :] = jnp.concatenate(out_b, axis=0).T.astype(BF16)


def attention_backward_kernel(
    p_ref,
    q_ref,
    k_ref,
    v_ref,
    ko_ref,
    vo_ref,
    do_ref,
    o_ref,
    lse_ref,
    f_ref,
    dq_ref,
    dk_ref,
    dv_ref,
    dko_ref,
    dvo_ref,
    g_ref,
    u_ref,
    acc_ref,
    dk_s,
    dv_s,
):
    half = p_ref[0]
    first = half == 1
    off = pl.multiple_of((1 - half) * 256, 256)
    base3 = pl.multiple_of(768 - half * 512, 256)
    q = q_ref[...].astype(F32) * 0.125
    do = do_ref[...].astype(F32)
    keep = causal()
    kt = k_ref[...].T
    kot = ko_ref[pl.ds(0, 256), :].T
    k5t = ko_ref[pl.ds(off, 256), :].T
    dk_s[...] = jnp.zeros_like(dk_s)
    dv_s[...] = jnp.zeros_like(dv_s)
    row8 = lax.broadcasted_iota(jnp.int32, (8, 128), 0)
    lane8 = lax.broadcasted_iota(jnp.int32, (8, 128), 1)
    ones = jnp.where(lane8 // 64 == row8, 1.0, 0.0)
    deltas = nt(ones, do * o_ref[...].astype(F32), precision=lax.Precision.HIGHEST)
    dqt_a, dqt_b = [], []
    for h in range(2):
        spread(u_ref, f_ref[0, h : h + 1, :])
        acc_ref[...] = jnp.zeros_like(acc_ref)
        qh = jnp.where(head_lanes(h), q, 0.0).astype(BF16)
        dh = jnp.where(head_lanes(h), do, 0.0).astype(BF16)
        lse = lse_ref[0, h : h + 1, :]
        delta = deltas[h : h + 1, :]
        rows = slice(64 * h, 64 * h + 64)

        def block(k, v, key_rows, k_t, qs, ds, l, d, base, masked):
            s = nt(k, qs) + toeplitz(u_ref, base)
            p = jnp.exp(s - l)
            if masked:
                p = jnp.where(keep, p, 0.0)
            e = p * (nt(v, ds) - d)
            acc_ref[:, pl.ds(pl.multiple_of(base + 256, 128), 256)] += e[:128]
            acc_ref[:, pl.ds(pl.multiple_of(base + 128, 128), 256)] += e[128:]
            el = e.astype(BF16)
            dv_s[key_rows, :] += nn(p.astype(BF16), ds)
            dk_s[key_rows, :] += nn(el, qs)
            return nn(k_t[rows], el)

        ka, kb = k_ref[pl.ds(0, 256), :], k_ref[pl.ds(256, 256), :]
        va, vb = v_ref[pl.ds(0, 256), :], v_ref[pl.ds(256, 256), :]
        qa, qb, da, db = qh[:256], qh[256:], dh[:256], dh[256:]
        la, lb, ea, eb = lse[:, :256], lse[:, 256:], delta[:, :256], delta[:, 256:]
        t1 = block(ka, va, pl.ds(0, 256), kt[:, :256], qa, da, la, ea, 0, True)
        t2 = block(kb, vb, pl.ds(256, 256), kt[:, 256:], qb, db, lb, eb, 0, True)
        t3 = block(ka, va, pl.ds(0, 256), kt[:, :256], qb, db, lb, eb, base3, False)
        t4 = block(
            ko_ref[pl.ds(0, 256), :],
            vo_ref[pl.ds(0, 256), :],
            pl.ds(512, 256),
            kot,
            qb,
            db,
            lb,
            eb,
            512,
            False,
        )
        t5 = block(
            ko_ref[pl.ds(off, 256), :],
            vo_ref[pl.ds(off, 256), :],
            pl.ds(pl.multiple_of(512 + off, 256), 256),
            k5t,
            jnp.where(first, qa, qb),
            jnp.where(first, da, db),
            jnp.where(first, la, lb),
            jnp.where(first, ea, eb),
            256,
            False,
        )
        dqt_a.append(t1 + jnp.where(first, t5, 0.0))
        dqt_b.append(t2 + t3 + t4 + jnp.where(first, 0.0, t5))
        x = acc_ref[...]
        width = x.shape[1]
        for r in (64, 32, 16, 8):
            x = x[:r] + pltpu.roll(x[r : 2 * r], width - r, 1)
        for r in (4, 2, 1):
            x = x + pltpu.roll(pltpu.roll(x, 8 - r, 0), width - r, 1)
        g_ref[0, h : h + 1, :] = x[0:1]
    dq_ref[pl.ds(0, 256), :] = (jnp.concatenate(dqt_a, axis=0).T * 0.125).astype(BF16)
    dq_ref[pl.ds(256, 256), :] = (jnp.concatenate(dqt_b, axis=0).T * 0.125).astype(BF16)
    dk_ref[...] = dk_s[pl.ds(0, 512), :]
    dv_ref[...] = dv_s[pl.ds(0, 512), :]
    dko_ref[...] = dk_s[pl.ds(512, 512), :].astype(BF16)
    dvo_ref[...] = dv_s[pl.ds(512, 512), :].astype(BF16)


def attention_specs(tokens, pairs):
    def at(column):
        return pl.BlockSpec((tokens, 128), lambda i, p, c=column: (0, c + i))

    def table(width):
        return pl.BlockSpec((1, 8, width), lambda i, p: (i, 0, 0))

    return at, table


def attention_forward(half, projected, other, distances):
    tokens, width = projected.shape[0], projected.shape[1] // 3
    pairs = width // 128
    at, table = attention_specs(tokens, pairs)
    return pl.pallas_call(
        attention_forward_kernel,
        grid_spec=pltpu.PrefetchScalarGridSpec(
            num_scalar_prefetch=1,
            grid=(pairs,),
            in_specs=[at(0), at(pairs), at(2 * pairs), at(0), at(pairs), table(1280)],
            out_specs=[at(0), table(tokens)],
            scratch_shapes=[pltpu.VMEM((128, 1280), F32)],
        ),
        out_shape=[
            jax.ShapeDtypeStruct((tokens, width), BF16),
            jax.ShapeDtypeStruct((pairs, 8, tokens), F32),
        ],
        cost_estimate=pl.CostEstimate(
            flops=int(4e9), bytes_accessed=6 << 20, transcendentals=tokens * 1024 * 10
        ),
        name="attention_forward",
    )(half, projected, projected, projected, other, other, distances)


def attention_backward(half, projected, other, d_mixed, mixed, lse, distances):
    tokens, width = mixed.shape
    pairs = width // 128
    at, table = attention_specs(tokens, pairs)
    wide = jax.ShapeDtypeStruct((tokens, width), F32)
    low = jax.ShapeDtypeStruct((tokens, width), BF16)
    return pl.pallas_call(
        attention_backward_kernel,
        grid_spec=pltpu.PrefetchScalarGridSpec(
            num_scalar_prefetch=1,
            grid=(pairs,),
            in_specs=[
                at(0),
                at(pairs),
                at(2 * pairs),
                at(0),
                at(pairs),
                at(0),
                at(0),
                table(tokens),
                table(1280),
            ],
            out_specs=[at(0)] * 5 + [table(1280)],
            scratch_shapes=[
                pltpu.VMEM((128, 1280), F32),
                pltpu.VMEM((128, 1280), F32),
                pltpu.VMEM((2 * tokens, 128), F32),
                pltpu.VMEM((2 * tokens, 128), F32),
            ],
        ),
        out_shape=[low, wide, wide, low, low, jax.ShapeDtypeStruct((pairs, 8, 1280), F32)],
        cost_estimate=pl.CostEstimate(
            flops=int(12e9), bytes_accessed=12 << 20, transcendentals=tokens * 1024 * 10
        ),
        name="attention_backward",
    )(half, projected, projected, projected, other, other, d_mixed, mixed, lse, distances)


MESH = pl.DeviceIdType.MESH
ORDER = (0, 4, 2, 6)


def flip(index, bit):
    return index + bit - 2 * bit * ((index // bit) % 2)


def flips(index, bits):
    for bit in (1, 2, 4):
        if bits & bit:
            index = flip(index, bit)
    return index


def fetch_kernel(
    qkv_ref,
    out_ref,
    small_ref,
    gu_ref,
    down_ref,
    qkv_full,
    out_full,
    small_full,
    gu_own,
    down_own,
    z_send,
    z_recv,
    g_send,
    g_recv,
    c_send,
    c_recv,
    w_send,
    w_recv,
    local,
):
    g, s = lax.axis_index("group"), lax.axis_index("shard")
    partners = [(flips(g, k), s) for k in (1, 2, 3)] + [(g, flip(s, b)) for b in (1, 2, 4)]
    barrier = pltpu.get_barrier_semaphore()
    for partner in partners:
        pl.semaphore_signal(barrier, inc=1, device_id=partner, device_id_type=MESH)
    pl.semaphore_wait(barrier, len(partners))

    owns = (qkv_ref, out_ref, small_ref)
    fulls = (qkv_full, out_full, small_full)
    copies, pending = [], {}

    def row(kg, j, core=0):
        return flips(g, kg) * 8 + flips(s, ORDER[j] + core)

    def send(src, dst, sems, index, device):
        copy = pltpu.make_async_remote_copy(
            src_ref=src,
            dst_ref=dst,
            send_sem=sems[0].at[index],
            recv_sem=sems[1].at[index],
            device_id=device,
            device_id_type=MESH,
        )
        copy.start()
        copies.append(copy)
        pending[id(copy)] = copy
        return copy

    def arrived(copy):
        copy.wait_recv()
        del pending[id(copy)]

    def source(a, kg, j):
        return owns[a] if kg == 0 and j == 0 else fulls[a].at[row(kg, j)]

    def to_z(a, j, bit, index):
        return send(
            source(a, 0, j), fulls[a].at[row(0, j)], (z_send, z_recv), (a, index), (g, flip(s, bit))
        )

    def to_groups(a, j):
        return [
            send(
                source(a, 0, j),
                fulls[a].at[row(0, j)],
                (g_send, g_recv),
                (a, k - 1, j),
                (flips(g, k), s),
            )
            for k in (1, 2, 3)
        ]

    def to_core(a, kg, j):
        return send(
            source(a, kg, j),
            fulls[a].at[row(kg, j)],
            (c_send, c_recv),
            (a, kg, j),
            (g, flip(s, 1)),
        )

    arrays = range(3)
    z = s // 2
    z_copies = [[to_z(a, 0, 4, 0), to_z(a, 0, 2, 1)] for a in arrays]
    in_plane = [to_groups(a, 0) for a in arrays]
    for a in arrays:
        to_core(a, 0, 0)
    spread_gu = [
        send(
            gu_ref.at[flips(g, k)],
            gu_own.at[g, z],
            (w_send, w_recv),
            (k - 1,),
            (flips(g, k), s),
        )
        for k in (1, 2, 3)
    ]
    mine = [
        pltpu.make_async_copy(owns[a], fulls[a].at[row(0, 0)], local.at[a]) for a in arrays
    ] + [
        pltpu.make_async_copy(gu_ref.at[g], gu_own.at[g, z], local.at[3]),
        pltpu.make_async_copy(down_ref.at[g], down_own.at[g, z], local.at[4]),
    ]
    for copy in mine:
        copy.start()
    plane = {(a, 0): in_plane[a] for a in arrays}
    for a in arrays:
        arrived(z_copies[a][0])
        z_copies[a].append(to_z(a, 1, 2, 2))
        plane[a, 1] = to_groups(a, 1)
        to_core(a, 0, 1)
    for a in arrays:
        arrived(z_copies[a][1])
        plane[a, 2] = to_groups(a, 2)
        to_core(a, 0, 2)
    for copy in spread_gu:
        arrived(copy)
    for copy in mine:
        copy.wait()
    for i, bit in enumerate((4, 2)):
        send(
            gu_own.at[:, z], gu_own.at[:, z], (w_send, w_recv), (6 + i,), (g, flip(s, bit))
        )
    for a in arrays:
        arrived(z_copies[a][2])
        plane[a, 3] = to_groups(a, 3)
        to_core(a, 0, 3)
    for k in (1, 2, 3):
        send(
            down_ref.at[flips(g, k)],
            down_own.at[g, z],
            (w_send, w_recv),
            (2 + k,),
            (flips(g, k), s),
        )
    for j in range(4):
        for a in arrays:
            for k in (1, 2, 3):
                arrived(plane[a, j][k - 1])
                to_core(a, k, j)
    for copy in list(pending.values()):
        arrived(copy)
    for copy in copies:
        copy.wait_send()


def fetch(qkv, out, small, gate_up, down):
    groups, shards = lax.axis_size("group"), lax.axis_size("shard")
    devices = groups * shards
    any_space = pl.BlockSpec(memory_space=pl.ANY)
    vmem = pl.BlockSpec(memory_space=pltpu.VMEM)
    dma = pltpu.SemaphoreType.DMA
    shapes = [
        jax.ShapeDtypeStruct((devices, *qkv.shape), BF16),
        jax.ShapeDtypeStruct((devices, *out.shape), BF16),
        jax.ShapeDtypeStruct((devices, *small.shape), BF16),
        jax.ShapeDtypeStruct((groups, shards // 2, *gate_up.shape[1:]), BF16),
        jax.ShapeDtypeStruct((groups, shards // 2, *down.shape[1:]), BF16),
    ]
    return pl.pallas_call(
        fetch_kernel,
        in_specs=[vmem] * 5,
        out_specs=[any_space] * 5,
        out_shape=shapes,
        scratch_shapes=[
            dma((3, 3)),
            dma((3, 3)),
            dma((3, 3, 4)),
            dma((3, 3, 4)),
            dma((3, 4, 4)),
            dma((3, 4, 4)),
            dma((8,)),
            dma((8,)),
            dma((5,)),
        ],
        compiler_params=pltpu.CompilerParams(collective_id=1, has_side_effects=True),
        cost_estimate=pl.CostEstimate(flops=0, bytes_accessed=24 << 20, transcendentals=0),
        name="fetch",
    )(qkv, out, small, gate_up, down)


def gelu_parts(v):
    c = 0.7978845608028654
    t = jnp.tanh(c * (v + 0.044715 * v * v * v))
    value = 0.5 * v * (1.0 + t)
    slope = 0.5 * (1.0 + t) + 0.5 * v * (1.0 - t * t) * c * (1.0 + 3 * 0.044715 * v * v)
    return value, slope


def join_rows(c, own_ref, sib_ref, gate_s, up_s):
    groups, zs, double, _ = own_ref.shape
    rows = double // 2
    for g in range(groups):
        for z in range(zs):
            for ref, core in ((own_ref, c), (sib_ref, 1 - c)):
                at = pl.multiple_of(((g * zs + z) * 2 + core) * rows, rows)
                gate_s[pl.ds(at, rows), :] = ref[g, z, :rows, :]
                up_s[pl.ds(at, rows), :] = ref[g, z, rows:, :]


def gate_up_kernel(joined, c_ref, x_ref, *refs):
    if joined:
        gate_s, up_s, hidden_ref, value_ref, factor_ref = refs
    else:
        own_ref, sib_ref, hidden_ref, value_ref, factor_ref, gate_s, up_s = refs
        join_rows(c_ref[0], own_ref, sib_ref, gate_s, up_s)
    step = 256
    for m in range(0, x_ref.shape[0], step):
        rows = pl.ds(m, step)
        gate_act = nn(x_ref[rows, :], gate_s[...])
        up_act = nn(x_ref[rows, :], up_s[...])
        value, slope = gelu_parts(gate_act)
        hidden_ref[rows, :] = (value * up_act).astype(BF16)
        value_ref[rows, :] = value.astype(BF16)
        factor_ref[rows, :] = (slope * up_act).astype(BF16)


def d_buffer_kernel(joined, c_ref, dg_ref, du_ref, *refs):
    if joined:
        gate_s, up_s, out_ref, acc_ref = refs
    else:
        own_ref, sib_ref, out_ref, acc_ref, gate_s, up_s = refs
        join_rows(c_ref[0], own_ref, sib_ref, gate_s, up_s)
    step = 256

    @pl.when(pl.program_id(0) == 0)
    def _():
        acc_ref[...] = jnp.zeros_like(acc_ref)

    for m in range(0, dg_ref.shape[0], step):
        rows = pl.ds(m, step)
        acc_ref[rows, :] += nt(dg_ref[rows, :], gate_s[...]) + nt(du_ref[rows, :], up_s[...])

    @pl.when(pl.program_id(0) == pl.num_programs(0) - 1)
    def _():
        out_ref[...] = acc_ref[...].astype(BF16)


TILE = 256


def weight_specs(weights):
    specs = []
    for w in weights:
        lead = w.shape[:-1]
        specs.append(pl.BlockSpec((*lead, TILE), lambda i, c, n=len(lead): (0,) * n + (i,)))
    return specs


def gate_up(core, x, weights):
    joined = weights[0].ndim == 2
    slots, width = x.shape
    ff = weights[0].shape[-1]
    tile = pl.BlockSpec((slots, TILE), lambda i, c: (0, i))
    scratch = [] if joined else [pltpu.VMEM((width, TILE), BF16)] * 2
    return pl.pallas_call(
        functools.partial(gate_up_kernel, joined),
        grid_spec=pltpu.PrefetchScalarGridSpec(
            num_scalar_prefetch=1,
            grid=(ff // TILE,),
            in_specs=[pl.BlockSpec((slots, width), lambda i, c: (0, 0)), *weight_specs(weights)],
            out_specs=[tile] * 3,
            scratch_shapes=scratch,
        ),
        out_shape=[jax.ShapeDtypeStruct((slots, ff), BF16)] * 3,
        cost_estimate=pl.CostEstimate(
            flops=4 * slots * width * ff, bytes_accessed=36 << 20, transcendentals=slots * ff
        ),
        name="gate_up",
    )(core, x, *weights)


def buffer_gradient(core, d_gate, d_up, weights):
    joined = weights[0].ndim == 2
    slots, ff = d_gate.shape
    width = weights[0].size // ff
    tile = pl.BlockSpec((slots, TILE), lambda i, c: (0, i))
    scratch = [pltpu.VMEM((slots, width), F32)]
    scratch += [] if joined else [pltpu.VMEM((width, TILE), BF16)] * 2
    return pl.pallas_call(
        functools.partial(d_buffer_kernel, joined),
        grid_spec=pltpu.PrefetchScalarGridSpec(
            num_scalar_prefetch=1,
            grid=(ff // TILE,),
            in_specs=[tile, tile, *weight_specs(weights)],
            out_specs=pl.BlockSpec((slots, width), lambda i, c: (0, 0)),
            scratch_shapes=scratch,
        ),
        out_shape=jax.ShapeDtypeStruct((slots, width), BF16),
        cost_estimate=pl.CostEstimate(
            flops=4 * slots * width * ff, bytes_accessed=28 << 20, transcendentals=0
        ),
        name="buffer_gradient",
    )(core, d_gate, d_up, *weights)


def place_kernel(m_ref, *refs):
    out_ref = refs[-1]
    for k in range(len(refs) - 1):

        @pl.when((pl.program_id(0) ^ m_ref[0]) == k)
        def _(k=k):
            out_ref[0] = refs[k][...].astype(F32)


def place(pieces, mine):
    rows, columns = pieces[0].shape
    count = len(pieces)
    whole = pl.BlockSpec((rows, columns), lambda i, m: (0, 0))
    return pl.pallas_call(
        place_kernel,
        grid_spec=pltpu.PrefetchScalarGridSpec(
            num_scalar_prefetch=1,
            grid=(count,),
            in_specs=[whole] * count,
            out_specs=pl.BlockSpec((1, rows, columns), lambda i, m: (i, 0, 0)),
        ),
        out_shape=jax.ShapeDtypeStruct((count, rows, columns), F32),
        cost_estimate=pl.CostEstimate(
            flops=0, bytes_accessed=6 * count * rows * columns, transcendentals=0
        ),
        name="place",
    )(mine.astype(jnp.int32).reshape(1), *pieces)


def gather_column(piece, axis):
    size = lax.axis_size(axis)
    me = lax.axis_index(axis)
    pieces = {0: piece}
    for bit in reversed(bits_of(size)):
        pieces.update({k | bit: swap(v, axis, bit) for k, v in list(pieces.items())})
    sources, rows, columns = piece.shape
    whole = jnp.zeros((sources, size, rows, columns), piece.dtype)
    for k, v in pieces.items():
        whole = lax.dynamic_update_slice(whole, v[:, None], (0, me ^ k, 0, 0))
    return whole.reshape(sources * size * rows, columns)


def to_experts(weight, experts):
    groups = lax.axis_size("group")
    sets = [[s * experts + i for i in range(experts)] for s in range(groups // experts)]
    moved = lax.all_to_all(
        weight,
        "group",
        split_axis=0,
        concat_axis=0,
        tiled=True,
        axis_index_groups=sets if len(sets) > 1 else None,
    )
    bit = experts
    me = lax.axis_index("group")
    while bit < groups:
        other = swap(moved, "group", bit)
        low = (me & bit) == 0
        moved = jnp.where(
            low, jnp.concatenate([moved, other]), jnp.concatenate([other, moved])
        )
        bit *= 2
    return moved


def pair_split(x, axis, width, bit_set):
    count = x.shape[axis] // width
    if axis == 0:
        view = x.reshape(count // 2, 2, width, *x.shape[1:])

        def half(bit):
            return lax.dynamic_index_in_dim(view, bit, 1, keepdims=False).reshape(
                count // 2 * width, *x.shape[1:]
            )

        return half(bit_set), half(1 - bit_set)

    def columns(bit):
        return jnp.concatenate(
            [
                lax.dynamic_slice_in_dim(x, (2 * m + bit) * width, width, axis)
                for m in range(count // 2)
            ],
            axis=axis,
        )

    return columns(bit_set), columns(1 - bit_set)


def halve(x, mesh_axis, bit, axis, width):
    me = lax.axis_index(mesh_axis)
    mine, theirs = pair_split(x, axis, width, jnp.where((me & bit) == 0, 0, 1))
    return (mine.astype(F32) + swap(theirs, mesh_axis, bit).astype(F32)).astype(x.dtype)


def reduce_column(grad, axis, width):
    for bit in bits_of(lax.axis_size("shard")):
        grad = halve(grad, "shard", bit, axis, width)
    return grad


def share_experts(part, experts):
    groups = lax.axis_size("group")
    me = lax.axis_index("group")
    bit = experts
    while bit < groups:
        part = (part.astype(F32) + swap(part, "group", bit).astype(F32)).astype(part.dtype)
        bit *= 2
    return place([part] + [swap(part, "group", k) for k in range(1, experts)], me % experts)


def reduce_dense(grad):
    shards = lax.axis_size("shard")
    groups = lax.axis_size("group")
    me = lax.axis_index("group")
    rows, columns = grad.shape
    width = rows // shards
    sub = width // groups
    x = halve(grad, "shard", 1, 0, width)
    view = x.reshape(shards // 2, groups, sub, columns)

    def part(which):
        return lax.dynamic_index_in_dim(view, which, 1, keepdims=False)

    total = part(me).astype(F32)
    for k in range(1, groups):
        total = total + swap(part(me ^ k), "group", k).astype(F32)
    x = total.astype(BF16).reshape(shards // 2 * sub, columns)
    for bit in bits_of(shards)[1:]:
        x = halve(x, "shard", bit, 0, sub)
    pieces = [x] + [swap(x, "group", k) for k in range(1, groups)]
    return place(pieces, me).reshape(width, columns)


def column_blocks(x, bit, part):
    count = x.shape[1] // part
    return jnp.concatenate(
        [
            lax.dynamic_slice_in_dim(x, (2 * m + bit) * part, part, 1)
            for m in range(count // 2)
        ],
        axis=1,
    )


def exchange(blocks, experts):
    return [blocks[0]] + [swap(blocks[k], "group", k) for k in range(1, experts)]


def norm_parts(x):
    inverse = lax.rsqrt(jnp.mean(x * x, axis=-1, keepdims=True) + EPSILON)
    return inverse


def norm_backward(d_out, x, inverse, gain):
    unit = x * inverse
    scaled = d_out * gain
    d_x = inverse * (scaled - unit * jnp.mean(scaled * unit, axis=-1, keepdims=True))
    return d_x, jnp.sum(d_out * unit, axis=0)


def on_device(
    inputs,
    cotangent,
    routes,
    priority,
    buckets,
    norm1_gain,
    qkv_weight,
    out_weight,
    rel_bias,
    norm2_gain,
    router_weight,
    gate_weight,
    up_weight,
    down_weight,
):
    tokens, width = inputs.shape
    experts = gate_weight.shape[0]
    ff = gate_weight.shape[2]
    both = ("group", "shard")
    devices = lax.axis_size("group") * lax.axis_size("shard")
    rows = qkv_weight.shape[0]
    shards = lax.axis_size("shard")

    bias_rows = jnp.pad(rel_bias.reshape(-1, 1), ((0, rows - rel_bias.shape[0]), (0, 0)))
    small = jnp.concatenate(
        [
            norm1_gain.reshape(rows, 1),
            norm2_gain.reshape(rows, 1),
            router_weight,
            bias_rows,
            jnp.zeros((rows, 128 - 3 - experts), BF16),
        ],
        axis=1,
    )
    groups = lax.axis_size("group")
    shard = lax.axis_index("shard")
    core = shard % 2
    gate_up_rows = jnp.concatenate([gate_weight, up_weight], axis=1)
    if groups == 4 and shards == 8:
        qkv_full, out_full, small_full, own, down_own = fetch(
            qkv_weight, out_weight, small, gate_up_rows, down_weight
        )
        qkv_full = qkv_full.reshape(width, 3 * width)
        out_full = out_full.reshape(width, width)
        small_full = small_full.reshape(width, 128)
        z = shard // 2
        forward = lax.dynamic_index_in_dim(own, z ^ 2, 1, keepdims=True)
        own = lax.dynamic_update_slice(own, swap(forward, "shard", 2), (0, z ^ 3, 0, 0))
        weights = (own, swap(own, "shard", 1))
        piece = lax.dynamic_index_in_dim(down_own, z, 1, keepdims=True)
        piece4, piece2 = swap(piece, "shard", 4), swap(piece, "shard", 2)
        for k, got in ((2, piece4), (1, piece2), (3, swap(piece4, "shard", 2))):
            down_own = lax.dynamic_update_slice(down_own, got, (0, z ^ k, 0, 0))
        down_sib = swap(down_own, "shard", 1)
        down_full = jnp.where(
            core == 0,
            jnp.stack([down_own, down_sib], axis=2),
            jnp.stack([down_sib, down_own], axis=2),
        ).reshape(ff, width)
    else:
        small_full = lax.all_gather(small, both, axis=0, tiled=True)
        qkv_full = lax.all_gather(qkv_weight, both, axis=0, tiled=True)
        out_full = lax.all_gather(out_weight, both, axis=0, tiled=True)
        pieces = to_experts(gate_up_rows, experts)
        weights = (
            gather_column(pieces[:, :rows], "shard"),
            gather_column(pieces[:, rows:], "shard"),
        )
        down_full = gather_column(to_experts(down_weight, experts), "shard")

    small_f32 = small_full.astype(F32)
    gain_one = small_f32[:, 0].reshape(1, width)
    gain_two = small_f32[:, 1].reshape(1, width)
    router_full = small_full[:, 2 : 2 + experts]
    per_device = rel_bias.shape[0]
    table = small_full[:, 2 + experts].reshape(devices, rows)[:, :per_device]
    table = table.reshape(BUCKETS, HEADS)

    padded = jnp.concatenate([jnp.full((256,), -1, jnp.int32), buckets])
    bucket_hot = padded[:, None] == jnp.arange(BUCKETS, dtype=jnp.int32)[None, :]
    distances = jnp.einsum(
        "bh,nb->hn", table, bucket_hot.astype(BF16), preferred_element_type=F32
    ).reshape(HEADS // 2, 2, 1280)
    distances = jnp.pad(distances, ((0, 0), (0, 6), (0, 0)))

    group = lax.axis_index("group")
    choices = 2 * tokens
    expert_of = routes.reshape(choices)
    ranking = priority.reshape(choices)
    expert_hot = expert_of[:, None] == jnp.arange(experts, dtype=jnp.int32)[None, :]
    earlier = (ranking[None, :] < ranking[:, None]).astype(BF16)
    counts = jnp.dot(earlier, expert_hot.astype(BF16), preferred_element_type=F32)
    slot = jnp.sum(jnp.where(expert_hot, counts, 0.0), axis=1).astype(jnp.int32)
    kept = slot < CAP
    slots = experts * CAP
    place = jnp.where(kept, (expert_of ^ (group % experts)) * CAP + slot, -1)
    place = place.reshape(tokens, 2)
    kept = kept.reshape(tokens, 2)
    slot_ids = jnp.arange(slots, dtype=jnp.int32)
    hot_rows = [place[:, c][:, None] == slot_ids[None, :] for c in range(2)]

    resid_in = inputs.astype(F32)
    inverse_one = norm_parts(resid_in)
    normed_one = (resid_in * inverse_one * gain_one).astype(BF16)
    projected = jnp.dot(normed_one, qkv_full, preferred_element_type=F32).astype(BF16)
    half = (lax.axis_index("shard") % 2).astype(jnp.int32).reshape(1)
    other = swap(projected[:, width:], "shard", 1)
    mixed, lse = attention_forward(half, projected, other, distances)
    resid_mid = resid_in + jnp.dot(mixed, out_full, preferred_element_type=F32)
    inverse_two = norm_parts(resid_mid)
    normed_two = (resid_mid * inverse_two * gain_two).astype(BF16)

    logits = jnp.dot(normed_two, router_full, preferred_element_type=F32)
    router_probs = jax.nn.softmax(logits, axis=1)
    route_hot = routes[:, :, None] == jnp.arange(experts, dtype=jnp.int32)[None, None, :]
    picked = jnp.sum(jnp.where(route_hot, router_probs[:, None, :], 0.0), axis=2)
    gates = jnp.where(kept, picked, 0.0)

    dispatch = (hot_rows[0] | hot_rows[1]).astype(BF16)
    buffer = jnp.einsum(
        "ts,td->sd", dispatch, normed_two, preferred_element_type=F32
    ).astype(BF16)
    slot_gates = jnp.sum(
        jnp.where(hot_rows[0], gates[:, 0:1], 0.0) + jnp.where(hot_rows[1], gates[:, 1:2], 0.0),
        axis=0,
    )
    d_slots = (
        jnp.einsum("ts,td->sd", dispatch, cotangent, preferred_element_type=F32)
        * slot_gates[:, None]
    ).astype(BF16)
    blocks = buffer.reshape(experts, CAP, width)
    x = jnp.concatenate(exchange(blocks, experts), axis=0)
    d_expert = jnp.concatenate(exchange(d_slots.reshape(experts, CAP, width), experts), axis=0)

    core_index = core.astype(jnp.int32).reshape(1)
    hidden, value, factor = gate_up(core_index, x, weights)
    expert_out = jnp.dot(hidden, down_full, preferred_element_type=F32).astype(BF16)
    returned = jnp.concatenate(
        exchange(expert_out.reshape(experts, CAP, width), experts), axis=0
    )
    part = width // shards

    def reduced(axis, product, sent, kept):
        got = swap(product(sent).astype(BF16), "shard", 1)
        grad = (product(kept) + got.astype(F32)).astype(BF16)
        for bit in bits_of(shards)[1:]:
            grad = halve(grad, "shard", bit, axis, part)
        return share_experts(grad, experts)

    d_sent, d_kept = [column_blocks(d_expert, bit, part) for bit in (1 - core, core)]
    x_sent, x_kept = [column_blocks(x, bit, part) for bit in (1 - core, core)]

    def product(a, b):
        return jnp.einsum("sa,sb->ab", a, b, preferred_element_type=F32)

    down_out = reduced(1, lambda d: product(hidden, d), d_sent, d_kept)
    d_hidden = jnp.einsum("sd,fd->sf", d_expert, down_full, preferred_element_type=F32)
    d_gate = (d_hidden * factor.astype(F32)).astype(BF16)
    d_up = (d_hidden * value.astype(F32)).astype(BF16)
    d_buffer = buffer_gradient(core_index, d_gate, d_up, weights)
    d_returned = jnp.concatenate(
        exchange(d_buffer.reshape(experts, CAP, width), experts), axis=0
    )
    gate_out = reduced(0, lambda a: product(a, d_gate), x_sent, x_kept)
    up_out = reduced(0, lambda a: product(a, d_up), x_sent, x_kept)

    grad_out = cotangent.astype(F32)
    mixture = jnp.zeros((tokens, width), F32)
    d_gates = []
    for c in range(2):
        rows_out = jnp.dot(hot_rows[c].astype(BF16), returned, preferred_element_type=F32)
        mixture = mixture + rows_out * gates[:, c : c + 1]
        d_gates.append(jnp.sum(grad_out * rows_out, axis=1))
    output = (resid_mid + mixture).astype(BF16)
    d_gates = jnp.stack(d_gates, axis=1)
    d_router = jnp.sum(jnp.where(route_hot, d_gates[:, :, None], 0.0), axis=1)
    d_logits = (
        router_probs * (d_router - jnp.sum(router_probs * d_router, axis=1, keepdims=True))
    ).astype(BF16)
    router_grad = jnp.einsum("td,te->ed", normed_two, d_logits, preferred_element_type=F32)
    d_normed_two = jnp.dot(dispatch, d_returned, preferred_element_type=F32) + jnp.einsum(
        "te,de->td", d_logits, router_full, preferred_element_type=F32
    )
    d_mid, gain_two_grad = norm_backward(d_normed_two, resid_mid, inverse_two, gain_two)
    d_resid_mid = grad_out + d_mid
    d_attn = d_resid_mid.astype(BF16)
    out_grad = reduce_dense(
        jnp.einsum("td,te->de", mixed, d_attn, preferred_element_type=F32).astype(BF16)
    )
    d_mixed = jnp.einsum("te,de->td", d_attn, out_full, preferred_element_type=F32).astype(BF16)
    dq, dk, dv, dk_other, dv_other, by_distance = attention_backward(
        half, projected, other, d_mixed, mixed, lse, distances
    )
    dk_back, dv_back = swap(dk_other, "shard", 1), swap(dv_other, "shard", 1)
    d_projected = jnp.concatenate(
        [dq, (dk + dk_back.astype(F32)).astype(BF16), (dv + dv_back.astype(F32)).astype(BF16)],
        axis=1,
    )
    qkv_grad = reduce_dense(
        jnp.einsum("td,te->de", normed_one, d_projected, preferred_element_type=F32).astype(BF16)
    )
    d_normed_one = jnp.einsum("te,de->td", d_projected, qkv_full, preferred_element_type=F32)
    d_in, gain_one_grad = norm_backward(d_normed_one, resid_in, inverse_one, gain_one)
    input_grad = d_resid_mid + d_in

    table_grad = jnp.einsum(
        "hn,nb->bh",
        by_distance[:, :2].reshape(HEADS, 1280),
        bucket_hot.astype(F32),
        preferred_element_type=F32,
        precision=lax.Precision.HIGHEST,
    ).reshape(1, BUCKETS * HEADS)
    packed = jnp.concatenate(
        [
            gain_one_grad.reshape(1, width),
            gain_two_grad.reshape(1, width),
            router_grad,
            jnp.pad(table_grad, ((0, 0), (0, width - BUCKETS * HEADS))),
            jnp.zeros((8 - 3 - experts, width), F32),
        ],
        axis=0,
    )
    packed = lax.psum(packed, both)
    own = lax.dynamic_slice_in_dim(packed, shard * part, part, 1)
    per_shard = BUCKETS * HEADS // shards
    rel_grad = lax.dynamic_slice(packed, (2 + experts, shard * per_shard), (1, per_shard))
    return (
        output,
        input_grad,
        own[0],
        qkv_grad,
        out_grad,
        rel_grad.reshape(per_shard),
        own[1],
        own[2 : 2 + experts].T,
        gate_out,
        up_out,
        down_out,
    )


def solution(mesh):
    return jax.shard_map(
        on_device,
        mesh=mesh,
        in_specs=(
            P(("group", "shard"), None),
            P(("group", "shard"), None),
            P(("group", "shard"), None),
            P(("group", "shard"), None),
            P(),
            P(("group", "shard")),
            P(("group", "shard"), None),
            P(("group", "shard"), None),
            P(("group", "shard")),
            P(("group", "shard")),
            P(("group", "shard"), None),
            P(None, ("group", "shard"), None),
            P(None, ("group", "shard"), None),
            P(None, ("group", "shard"), None),
        ),
        out_specs=(
            P(("group", "shard"), None),
            P(("group", "shard"), None),
            P("shard"),
            P("shard", None),
            P("shard", None),
            P("shard"),
            P("shard"),
            P("shard", None),
            P(None, "shard", None),
            P(None, "shard", None),
            P(None, None, "shard"),
        ),
        check_vma=False,
    )
```
